32 devices in a mesh: gx: 8 (over z, y), gy: 4 (over x, core).
Axes of the slice: x: 2, y: 2, z: 4, core: 2. Of those that a mesh axis runs over, the one named last changes fastest.
Arguments:
- goal_embed: bfloat16 [4096, 128], P(('gx', 'gy')), may hold values from -6 to 6
- goal_bins: int32 [4096], P(('gx', 'gy')), may hold values from 0 to 2047, as said below
- goal_weights: float32 [4096], P(('gx', 'gy')), may hold values from 0.1 to 10
Outputs:
- bin_mean: float32 [2048, 128], P(('gx', 'gy'))
- rarity: float32 [2048], P(('gx', 'gy'))
The draws below stay inside these ranges and needn't reach their ends.
Inputs may be any that keep to these rules, and one draw needn't show every extreme that they name: `goal_bins`: bin b belongs to owner b // 64, owners numbered in the order of gx then gy. Of the goals of one device, at most 8 fall in the bins of one owner; some owner receives exactly 8 goals from every device.
All inputs are finite; a program needn't handle non-finite values.
Results may differ from the reference program's by a relative error of at most 0.0029.
Values may be sent and summed in bfloat16 or wider, within the bound.
A program may use at most 64 MiB of HBM per device.

```python
import math
import jax
import jax.numpy as jnp

E = 128
BINS_DEV = 64
G_DEV = 128
GOALS = 4096
BINS = 2048
N_GX = 8
N_GY = 4


def draw_goal_bins(key, part):
    devices = N_GX * N_GY
    capacity = max(2, 2 * G_DEV // devices)
    key_common = jax.random.fold_in(key, 11)
    key_blocks = jax.random.fold_in(key, 12)
    key_offset = jax.random.fold_in(key, 13)
    common = jax.random.randint(key_common, (), 0, devices).astype(jnp.int32)

    def one_block(block_key):
        key_slots = jax.random.fold_in(block_key, 1)
        key_order = jax.random.fold_in(block_key, 2)
        slots = jax.random.permutation(key_slots, (devices - 1) * capacity).astype(jnp.int32)
        others = slots[:G_DEV - capacity] // capacity
        others = others + (others >= common).astype(jnp.int32)
        owners = jnp.concatenate([jnp.zeros((capacity,), jnp.int32) + common, others.astype(jnp.int32)])
        return jax.random.permutation(key_order, owners).astype(jnp.int32)
    owners = jax.vmap(one_block)(jax.random.split(key_blocks, devices)).reshape(-1)
    offsets = jax.random.randint(key_offset, (G_DEV * devices,), 0, BINS_DEV).astype(jnp.int32)
    return (owners * BINS_DEV + offsets).astype(jnp.int32)


def steps_of(rng, extent, pieces, least, high):
    gain = 1.0
    for position, shards_of in pieces:
        draws = jax.random.uniform(jax.random.fold_in(jax.random.fold_in(rng, 6), position), (shards_of,), jnp.float32, least / len(pieces), high / len(pieces))
        gain = gain * jnp.repeat(jnp.exp(draws), extent[position] // shards_of).reshape((-1,) + (1,) * (len(extent) - 1 - position))
    return gain


def gaussian(stream_key, dims, spread, reach, cuts=(), kind=jnp.bfloat16):
    array = jax.random.normal(stream_key, dims, jnp.float32) * spread
    if len(cuts) > 0:
        array = steps_of(stream_key, dims, cuts, -0.22, 0.18) * array
    return jnp.clip(array, min=-reach, max=reach).astype(kind)


def setup_inputs(seed: int = 0) -> dict:
    streams_of = jax.random.split(jax.random.key(seed), 4)
    goal_embed = gaussian(streams_of[0], (GOALS, E), 1.0, 6.0, ((0, 32),))
    goal_bins = draw_goal_bins(jax.random.fold_in(streams_of[3], 71), 0)
    goal_weights = jnp.clip(jnp.exp(math.log(10.0) - 4.6051702 * jax.random.uniform(streams_of[2], (GOALS,), jnp.float32) ** steps_of(streams_of[2], (GOALS,), ((0, 32),), -0.2, 0.2)), 0.1, 10.0)
    return {"goal_embed": goal_embed, "goal_bins": goal_bins, "goal_weights": goal_weights}


def reference(goal_embed, goal_bins, goal_weights):
    scaled = (goal_weights[:, None] * goal_embed.astype(jnp.float32)).astype(jnp.bfloat16)
    bin_sums = jax.ops.segment_sum(scaled.astype(jnp.float32), goal_bins, num_segments=BINS)
    bin_mass = jax.ops.segment_sum(goal_weights, goal_bins, num_segments=BINS)
    total_mass = jnp.sum(goal_weights)
    bin_mean = bin_sums / (bin_mass[:, None] + 1.0)
    rarity = jnp.log(total_mass / BINS) - jnp.log(bin_mass + 1.0)
    return bin_mean, rarity
```

```python
import functools

import jax
import jax.numpy as jnp
from jax import lax
from jax.experimental import pallas as pl
from jax.experimental.pallas import tpu as pltpu
from jax.sharding import PartitionSpec as P

BINS_DEV = 64
MARKS = 4
LATE = 4
LOGICAL = pl.DeviceIdType.LOGICAL


def each(first, last, body):
    if last - first <= 64:
        for k in range(first, last):
            body(k)
    else:
        lax.fori_loop(first, last, lambda k, c: (body(k), c)[1], 0)


def split3(x):
    hi = x.astype(jnp.bfloat16).astype(jnp.float32)
    rest = x - hi
    mid = rest.astype(jnp.bfloat16).astype(jnp.float32)
    return hi, mid, rest - mid


def split2(x):
    hi = x.astype(jnp.bfloat16).astype(jnp.float32)
    return hi, x - hi


def kernel(across, along, stride, embed_hbm, bins_hbm, weights_hbm, mean_ref, rarity_ref, send, recv, send_sem, recv_sem, gate, embed_ref, bins_ref, weights_ref, in_sem):
    loads = [pltpu.make_async_copy(a, b, in_sem.at[i]) for i, (a, b) in enumerate(((bins_hbm, bins_ref), (weights_hbm, weights_ref), (embed_hbm, embed_ref)))]
    for c in loads:
        c.start()
    n = across * along
    goals, width = embed_ref.shape
    sent_rows = stride + MARKS
    me = lax.axis_index("gx") * along + lax.axis_index("gy")

    late = min(LATE, n // 2)
    early = n - late
    is_late = me >= early

    def signal(sem, d):
        pl.semaphore_signal(sem, inc=1, device_id=d, device_id_type=LOGICAL)

    barrier = pltpu.get_barrier_semaphore()
    each(0, n, lambda d: pl.when((me != d) & (me < early))(lambda: signal(barrier, d)))

    loads[0].wait()
    loads[1].wait()
    bins = bins_ref[...]
    weights = weights_ref[...]
    shift = BINS_DEV.bit_length() - 1
    owners = lax.shift_right_logical(bins, shift)
    labels = (bins - owners * BINS_DEV).astype(jnp.float32)
    owners_col = jnp.broadcast_to(owners, (goals, goals)).T
    weights_col = jnp.broadcast_to(weights, (goals, goals)).T
    sub = lax.broadcasted_iota(jnp.int32, (goals, goals), 0)
    lane = lax.broadcasted_iota(jnp.int32, (goals, goals), 1)
    earlier = (owners_col == owners) & (sub < lane)
    place = jnp.sum(earlier.astype(jnp.float32), axis=0, keepdims=True).astype(jnp.int32)
    loads[2].wait()
    rows_iota = lax.broadcasted_iota(jnp.int32, (n * stride, goals), 0)
    pick = (rows_iota == owners * stride + place).astype(jnp.bfloat16)
    group = lax.shift_right_logical(rows_iota, stride.bit_length() - 1) == owners
    hi, lo = split2(weights)
    t_sub = lax.broadcasted_iota(jnp.int32, (stride, goals), 0)
    t_lane = lax.broadcasted_iota(jnp.int32, (stride, goals), 1)
    kinds = jnp.where(t_sub == 0, labels, jnp.where(t_sub == 1, hi, jnp.where(t_sub == 2, lo, 0.0)))
    kinds = jnp.broadcast_to(kinds[None], (n, stride, goals)).reshape(n * stride, goals)
    tagged = jnp.where(group, kinds, 0.0).astype(jnp.bfloat16)
    base = lax.rem(me, goals // stride) * stride
    spot = (sub == place + base).astype(jnp.bfloat16)
    marks = lax.dot_general(tagged, spot, (((1,), (1,)), ((), ())), preferred_element_type=jnp.float32)
    local = jnp.sum(weights, axis=1, keepdims=True)
    total = jnp.zeros((stride, goals), jnp.float32)
    for i, part in enumerate(split3(local)):
        total = jnp.where((t_sub == 3) & (t_lane == i), part, total)
    marks = marks.reshape(n, stride, goals) + total[None]
    scaled = (weights_col[:, :width] * embed_ref[...].astype(jnp.float32)).astype(jnp.bfloat16)
    rows = jnp.dot(pick, scaled, preferred_element_type=jnp.float32)
    send[...] = jnp.concatenate([rows.reshape(n, stride, width), marks], axis=1).astype(jnp.bfloat16)

    def start(d):
        pltpu.make_async_remote_copy(
            src_ref=send.at[d, pl.ds(0, sent_rows)],
            dst_ref=recv.at[me, pl.ds(0, sent_rows)],
            send_sem=send_sem,
            recv_sem=recv_sem,
            device_id=d,
            device_id_type=LOGICAL,
        ).start()

    pl.semaphore_wait(barrier, jnp.where(is_late, early, early - 1))
    pl.when(is_late)(lambda: each(0, early, lambda d: signal(gate, d)))
    each(0, early, lambda d: pl.when(me != d)(lambda: start(d)))
    pl.semaphore_wait(gate, jnp.where(is_late, 1, late))
    each(early, n, lambda d: pl.when(me == d - late)(lambda: signal(gate, d)))
    each(early, n, lambda d: pl.when(me != d)(lambda: start(d)))
    recv[me] = send[me]
    landed = recv.at[pl.ds(0, n - 1), pl.ds(0, sent_rows)]
    pltpu.make_async_copy(landed, landed, recv_sem).wait()

    data = recv[...].astype(jnp.float32)
    values = data[:, :stride].reshape(n * stride, width).astype(jnp.bfloat16)
    tags = data[:, stride:]
    per = goals // stride
    r_sub = lax.broadcasted_iota(jnp.int32, (BINS_DEV, goals), 0)
    r_lane = lax.broadcasted_iota(jnp.int32, (BINS_DEV, goals), 1)
    mass = jnp.zeros((BINS_DEV, goals), jnp.float32)
    chosen = []
    total = jnp.zeros((1, goals), jnp.float32)
    for q in range(0, n, per):
        added = jnp.sum(tags[q : q + per], axis=0)
        hit = r_sub == added[0:1].astype(jnp.int32)
        chosen.append(jnp.where(hit, 1.0, 0.0).astype(jnp.bfloat16))
        mass = mass + jnp.where(hit, added[1:2] + added[2:3], 0.0)
        total = total + added[3:4]
    choose = jnp.concatenate(chosen, axis=1)[:, : n * stride]
    sums = jnp.dot(choose, values, preferred_element_type=jnp.float32)
    mass_col = jnp.sum(mass, axis=1, keepdims=True) + 1.0
    total = jnp.sum(total, axis=1, keepdims=True)
    mean_ref[...] = sums * (1.0 / mass_col)
    mass_row = jnp.sum(jnp.where(r_sub == r_lane, mass_col, 0.0), axis=0, keepdims=True)
    rarity_ref[...] = (jnp.log(total / (BINS_DEV * n)) - jnp.log(mass_row))[:, :BINS_DEV]
    sent = send.at[pl.ds(0, n - 1), pl.ds(0, sent_rows)]
    pltpu.make_async_copy(sent, sent, send_sem).wait()


def put(mean, rarity, mean_hbm, rarity_hbm, sem):
    copies = [pltpu.make_async_copy(mean, mean_hbm, sem.at[0]), pltpu.make_async_copy(rarity, rarity_hbm, sem.at[1])]
    for c in copies:
        c.start()
    for c in copies:
        c.wait()


def shards(goal_embed, goal_bins, goal_weights):
    goals, width = goal_embed.shape
    across = lax.axis_size("gx")
    along = lax.axis_size("gy")
    n = across * along
    capacity = max(2, 2 * goals // n)
    stride = -(-capacity // 8) * 8
    mean, rarity = pl.pallas_call(
        functools.partial(kernel, across, along, stride),
        out_shape=(
            pltpu.VMEM((BINS_DEV, width), jnp.float32),
            pltpu.VMEM((1, BINS_DEV), jnp.float32),
        ),
        in_specs=[pl.BlockSpec(memory_space=pl.ANY)] * 3,
        out_specs=(pl.BlockSpec(memory_space=pltpu.VMEM),) * 2,
        scratch_shapes=[
            pltpu.VMEM((n, 2 * stride, width), jnp.bfloat16),
            pltpu.VMEM((n, 2 * stride, width), jnp.bfloat16),
            pltpu.SemaphoreType.DMA,
            pltpu.SemaphoreType.DMA,
            pltpu.SemaphoreType.REGULAR,
            pltpu.VMEM((goals, width), jnp.bfloat16),
            pltpu.VMEM((1, goals), jnp.int32),
            pltpu.VMEM((1, goals), jnp.float32),
            pltpu.SemaphoreType.DMA((3,)),
        ],
        compiler_params=pltpu.CompilerParams(collective_id=0, has_side_effects=True),
    )(goal_embed, goal_bins.reshape(1, goals), goal_weights.reshape(1, goals))
    mean, rarity = pl.pallas_call(
        put,
        out_shape=(
            jax.ShapeDtypeStruct((BINS_DEV, width), jnp.float32),
            jax.ShapeDtypeStruct((1, BINS_DEV), jnp.float32),
        ),
        in_specs=[pl.BlockSpec(memory_space=pltpu.VMEM)] * 2,
        out_specs=(pl.BlockSpec(memory_space=pl.ANY),) * 2,
        scratch_shapes=[pltpu.SemaphoreType.DMA((2,))],
    )(pltpu.with_memory_space_constraint(mean, pltpu.VMEM), pltpu.with_memory_space_constraint(rarity, pltpu.VMEM))
    return mean, rarity.reshape(BINS_DEV)


def solution(mesh):
    in_specs = (P(("gx", "gy"), None), P(("gx", "gy")), P(("gx", "gy")))
    out_specs = (P(("gx", "gy"), None), P(("gx", "gy")))
    return jax.shard_map(shards, mesh=mesh, in_specs=in_specs, out_specs=out_specs, check_vma=False)
```

```python
import functools

import jax
import jax.numpy as jnp
from jax import lax
from jax.experimental import pallas as pl
from jax.experimental.pallas import tpu as pltpu
from jax.sharding import PartitionSpec as P

BINS_DEV = 64
MARKS = 4
LATE = 6
LOGICAL = pl.DeviceIdType.LOGICAL


def each(first, last, body):
    if last - first <= 64:
        for k in range(first, last):
            body(k)
    else:
        lax.fori_loop(first, last, lambda k, c: (body(k), c)[1], 0)


def split2(x):
    hi = x.astype(jnp.bfloat16).astype(jnp.float32)
    return hi, x - hi


def split3(x):
    hi, rest = split2(x)
    mid, low = split2(rest)
    return hi, mid, low


def tree(parts):
    while len(parts) > 1:
        parts = [sum(parts[i : i + 2]) for i in range(0, len(parts), 2)]
    return parts[0]


def kernel(across, along, stride, embed_hbm, bins_hbm, weights_hbm, mean_ref, rarity_ref, send, recv, send_sem, recv_sem, gate, embed_ref, pair_ref, in_sem, bins_ref, weights_ref):
    pltpu.make_async_copy(bins_hbm, bins_ref, in_sem).start()
    pltpu.make_async_copy(weights_hbm, weights_ref, in_sem).start()
    embed_load = pltpu.make_async_copy(embed_hbm, embed_ref, send_sem)
    embed_load.start()
    n = across * along
    goals, width = embed_ref.shape
    sent_rows = stride + MARKS
    me = lax.axis_index("gx") * along + lax.axis_index("gy")
    late = min(LATE, n // 2)
    early = n - late
    is_late = me >= early

    def signal(sem, d):
        pl.semaphore_signal(sem, inc=1, device_id=d, device_id_type=LOGICAL)

    barrier = pltpu.get_barrier_semaphore()
    each(0, n, lambda d: pl.when((me != d) & (me < early))(lambda: signal(barrier, d)))

    shift = BINS_DEV.bit_length() - 1
    sub = lax.broadcasted_iota(jnp.int32, (goals, goals), 0)
    lane = lax.broadcasted_iota(jnp.int32, (goals, goals), 1)
    rows_iota = lax.broadcasted_iota(jnp.int32, (n * stride, goals), 0)
    t_sub = lax.broadcasted_iota(jnp.int32, (stride, goals), 0)
    t_lane = lax.broadcasted_iota(jnp.int32, (stride, goals), 1)
    before = (sub < lane).astype(jnp.bfloat16)
    pltpu.make_async_copy(pair_ref, pair_ref, in_sem).wait()
    bins = bins_ref[...]
    weights = weights_ref[...]
    owners = lax.shift_right_logical(bins, shift)
    labels = (bins - owners * BINS_DEV).astype(jnp.float32)
    hi, lo = split2(weights)
    owners_row = jnp.broadcast_to(owners.astype(jnp.float32), (goals, goals)).astype(jnp.bfloat16)
    same = jnp.where(owners_row.T == owners_row, before, jnp.bfloat16(0))
    same = tree([same[i : i + 16] for i in range(0, goals, 16)])
    place = jnp.sum(same.astype(jnp.float32), axis=0, keepdims=True).astype(jnp.int32)
    weights_col = jnp.broadcast_to(weights, (goals, goals)).T
    embed_load.wait()
    base = lax.rem(me, goals // stride) * stride
    spot = (sub == place + base).astype(jnp.bfloat16)
    kind = lax.rem(t_sub, MARKS)
    kinds = jnp.where(kind == 0, labels, jnp.where(kind == 1, hi, jnp.where(kind == 2, lo, 0.0)))
    half = n // 2
    owner_of = jnp.where(t_sub < MARKS, 0, half)
    tagged = jnp.concatenate([jnp.where(owner_of + o == owners, kinds, 0.0) for o in range(half)], axis=0).astype(jnp.bfloat16)
    marks = lax.dot_general(tagged, spot, (((1,), (1,)), ((), ())), preferred_element_type=jnp.float32)
    marks = marks.reshape(half, stride, goals)
    marks = jnp.concatenate([marks, jnp.roll(marks, -MARKS, axis=1)], axis=0)
    scaled = (weights_col[:, :width] * embed_ref[...].astype(jnp.float32)).astype(jnp.bfloat16)
    pick = (rows_iota == owners * stride + place).astype(jnp.bfloat16)
    rows = jnp.dot(pick, scaled, preferred_element_type=jnp.float32)
    local = jnp.sum(weights, axis=1, keepdims=True)
    total = jnp.zeros((stride, goals), jnp.float32)
    for i, part in enumerate(split3(local)):
        total = jnp.where((t_sub == 3) & (t_lane == i), part, total)
    marks = marks + total[None]
    send[...] = jnp.concatenate([rows.reshape(n, stride, width), marks], axis=1).astype(jnp.bfloat16)

    def start(d):
        pltpu.make_async_remote_copy(
            src_ref=send.at[d, pl.ds(0, sent_rows)],
            dst_ref=recv.at[me, pl.ds(0, sent_rows)],
            send_sem=send_sem,
            recv_sem=recv_sem,
            device_id=d,
            device_id_type=LOGICAL,
        ).start()

    pl.semaphore_wait(barrier, jnp.where(is_late, early, early - 1))
    each(0, early, lambda d: pl.when(me != d)(lambda: start(d)))
    pl.when(is_late)(lambda: each(0, early, lambda d: signal(gate, d)))
    pl.semaphore_wait(gate, jnp.where(is_late, 1, late))
    each(early, n, lambda d: pl.when(me == d - late)(lambda: signal(gate, d)))
    each(early, n, lambda d: pl.when(me != d)(lambda: start(d)))
    recv[me] = send[me]
    landed = recv.at[pl.ds(0, n - 1), pl.ds(0, sent_rows)]
    pltpu.make_async_copy(landed, landed, recv_sem).wait()

    data = recv[...].astype(jnp.float32)
    values = data[:, :stride].reshape(n * stride, width).astype(jnp.bfloat16)
    tags = data[:, stride:]
    per = goals // stride
    r_sub = lax.broadcasted_iota(jnp.int32, (BINS_DEV, goals), 0)
    r_lane = lax.broadcasted_iota(jnp.int32, (BINS_DEV, goals), 1)
    bin_of = r_sub.astype(jnp.float32)
    masses, chosen, totals = [], [], []
    for q in range(0, n, per):
        added = tree([tags[s] for s in range(q, min(q + per, n))])
        hit = bin_of == added[0:1]
        chosen.append(jnp.where(hit, 1.0, 0.0).astype(jnp.bfloat16))
        masses.append(jnp.where(hit, added[1:2] + added[2:3], 0.0))
        totals.append(added[3:4])
    choose = jnp.concatenate(chosen, axis=1)[:, : n * stride]
    sums = jnp.dot(choose, values, preferred_element_type=jnp.float32)
    mass_col = jnp.sum(tree(masses), axis=1, keepdims=True) + 1.0
    total = jnp.sum(tree(totals), axis=1, keepdims=True)
    mean_ref[...] = sums * (1.0 / mass_col)
    mass_row = jnp.sum(jnp.where(r_sub == r_lane, mass_col, 0.0), axis=0, keepdims=True)
    rarity_ref[...] = (jnp.log(total / (BINS_DEV * n)) - jnp.log(mass_row))[:, :BINS_DEV]
    sent = send.at[pl.ds(0, n - 1), pl.ds(0, sent_rows)]
    pltpu.make_async_copy(sent, sent, send_sem).wait()


def put(mean, rarity, mean_hbm, rarity_hbm, sem):
    copies = [pltpu.make_async_copy(mean, mean_hbm, sem.at[0]), pltpu.make_async_copy(rarity, rarity_hbm, sem.at[1])]
    for c in copies:
        c.start()
    for c in copies:
        c.wait()


def shards(goal_embed, goal_bins, goal_weights):
    goals, width = goal_embed.shape
    across = lax.axis_size("gx")
    along = lax.axis_size("gy")
    n = across * along
    capacity = max(2, 2 * goals // n)
    stride = -(-capacity // 8) * 8
    mean, rarity = pl.pallas_call(
        functools.partial(kernel, across, along, stride),
        out_shape=(
            pltpu.VMEM((BINS_DEV, width), jnp.float32),
            pltpu.VMEM((1, BINS_DEV), jnp.float32),
        ),
        in_specs=[pl.BlockSpec(memory_space=pl.ANY)] * 3,
        out_specs=(pl.BlockSpec(memory_space=pltpu.VMEM),) * 2,
        scratch_shapes=[
            pltpu.VMEM((n, 2 * stride, width), jnp.bfloat16),
            pltpu.VMEM((n, 2 * stride, width), jnp.bfloat16),
            pltpu.SemaphoreType.DMA,
            pltpu.SemaphoreType.DMA,
            pltpu.SemaphoreType.REGULAR,
            pltpu.VMEM((goals, width), jnp.bfloat16),
            pltpu.VMEM((2, goals), jnp.float32),
            pltpu.SemaphoreType.DMA,
            pltpu.VMEM((1, goals), jnp.int32),
            pltpu.VMEM((1, goals), jnp.float32),
        ],
        compiler_params=pltpu.CompilerParams(collective_id=0, has_side_effects=True),
    )(goal_embed, goal_bins.reshape(1, goals), goal_weights.reshape(1, goals))
    mean, rarity = pl.pallas_call(
        put,
        out_shape=(
            jax.ShapeDtypeStruct((BINS_DEV, width), jnp.float32),
            jax.ShapeDtypeStruct((1, BINS_DEV), jnp.float32),
        ),
        in_specs=[pl.BlockSpec(memory_space=pltpu.VMEM)] * 2,
        out_specs=(pl.BlockSpec(memory_space=pl.ANY),) * 2,
        scratch_shapes=[pltpu.SemaphoreType.DMA((2,))],
    )(pltpu.with_memory_space_constraint(mean, pltpu.VMEM), pltpu.with_memory_space_constraint(rarity, pltpu.VMEM))
    return mean, rarity.reshape(BINS_DEV)


def solution(mesh):
    in_specs = (P(("gx", "gy"), None), P(("gx", "gy")), P(("gx", "gy")))
    out_specs = (P(("gx", "gy"), None), P(("gx", "gy")))
    return jax.shard_map(shards, mesh=mesh, in_specs=in_specs, out_specs=out_specs, check_vma=False)
```

```python
import functools

import jax
import jax.numpy as jnp
from jax import lax
from jax.experimental import pallas as pl
from jax.experimental.pallas import tpu as pltpu
from jax.sharding import PartitionSpec as P

BINS_DEV = 64
MARKS = 4
LATE = 6
LEAD = 8
LOGICAL = pl.DeviceIdType.LOGICAL


def each(first, last, body):
    if last - first <= 64:
        for k in range(first, last):
            body(k)
    else:
        lax.fori_loop(first, last, lambda k, c: (body(k), c)[1], 0)


def split2(x):
    hi = x.astype(jnp.bfloat16).astype(jnp.float32)
    return hi, x - hi


def split3(x):
    hi, rest = split2(x)
    mid, low = split2(rest)
    return hi, mid, low


def tree(parts):
    while len(parts) > 1:
        parts = [sum(parts[i : i + 2]) for i in range(0, len(parts), 2)]
    return parts[0]


def kernel(across, along, stride, embed_hbm, bins_hbm, weights_hbm, mean_ref, rarity_ref, send, recv, send_sem, recv_sem, gate, embed_ref, pair_ref, in_sem, bins_ref, weights_ref):
    n = across * along
    goals, width = embed_ref.shape
    for i in range(1):
        part = pl.ds(i * (goals // 1), goals // 1)
        pltpu.make_async_copy(embed_hbm.at[part], embed_ref.at[part], send_sem).start()
    pltpu.make_async_copy(bins_hbm, bins_ref, in_sem).start()
    pltpu.make_async_copy(weights_hbm, weights_ref, in_sem).start()
    embed_load = pltpu.make_async_copy(embed_hbm, embed_ref, send_sem)
    sent_rows = stride + MARKS
    me = lax.axis_index("gx") * along + lax.axis_index("gy")
    late = min(LATE, n // 2)
    early = n - late
    is_late = me >= early

    def signal(sem, d):
        pl.semaphore_signal(sem, inc=1, device_id=d, device_id_type=LOGICAL)

    barrier = pltpu.get_barrier_semaphore()
    each(0, n, lambda d: pl.when((me != d) & (me < early))(lambda: signal(barrier, d)))

    shift = BINS_DEV.bit_length() - 1
    sub = lax.broadcasted_iota(jnp.int32, (goals, goals), 0)
    lane = lax.broadcasted_iota(jnp.int32, (goals, goals), 1)
    t_sub = lax.broadcasted_iota(jnp.int32, (stride, goals), 0)
    t_lane = lax.broadcasted_iota(jnp.int32, (stride, goals), 1)
    exact = jnp.bfloat16 if n <= 256 else jnp.float32
    before = (sub < lane).astype(exact)
    pltpu.make_async_copy(pair_ref, pair_ref, in_sem).wait()
    bins = bins_ref[...]
    weights = weights_ref[...]
    owners = lax.shift_right_logical(bins, shift)
    labels = (bins - owners * BINS_DEV).astype(jnp.float32)
    hi, lo = split2(weights)
    owners_row = jnp.broadcast_to(owners.astype(jnp.float32), (goals, goals)).astype(exact)
    same = jnp.where(owners_row.T == owners_row, before, exact(0))
    same = tree([same[i : i + 16] for i in range(0, goals, 16)])
    place = jnp.sum(same.astype(jnp.float32), axis=0, keepdims=True).astype(jnp.int32)
    weights_col = jnp.broadcast_to(weights, (goals, goals)).T
    embed_load.wait()
    base = lax.rem(me, goals // stride) * stride
    spot = (sub == place + base).astype(jnp.bfloat16)
    slot = owners * stride + place
    kind = lax.rem(t_sub, MARKS)
    kinds = jnp.where(kind == 0, labels, jnp.where(kind == 1, hi, jnp.where(kind == 2, lo, 0.0)))
    scaled = (weights_col[:, :width] * embed_ref[...].astype(jnp.float32)).astype(jnp.bfloat16)
    local = jnp.sum(weights, axis=1, keepdims=True)
    total = jnp.zeros((stride, goals), jnp.float32)
    for i, part in enumerate(split3(local)):
        total = jnp.where((t_sub == 3) & (t_lane == i), part, total)

    def pack(first, count):
        half = count // 2
        rows_iota = lax.broadcasted_iota(jnp.int32, (count * stride, goals), 0) + first * stride
        rows = jnp.dot((rows_iota == slot).astype(jnp.bfloat16), scaled, preferred_element_type=jnp.float32)
        owner_of = jnp.where(t_sub < MARKS, first, first + half)
        tagged = [jnp.where(owner_of + o == owners, kinds, 0.0) for o in range(half)]
        tagged = jnp.concatenate(tagged, axis=0).astype(jnp.bfloat16)
        marks = lax.dot_general(tagged, spot, (((1,), (1,)), ((), ())), preferred_element_type=jnp.float32)
        marks = marks.reshape(half, stride, goals)
        marks = jnp.concatenate([marks, jnp.roll(marks, -MARKS, axis=1)], axis=0) + total[None]
        both = jnp.concatenate([rows.reshape(count, stride, width), marks], axis=1)
        send[first : first + count] = both.astype(jnp.bfloat16)

    lead = min(LEAD, early)
    pack(0, lead)

    def start(d):
        pltpu.make_async_remote_copy(
            src_ref=send.at[d, pl.ds(0, sent_rows)],
            dst_ref=recv.at[me, pl.ds(0, sent_rows)],
            send_sem=send_sem,
            recv_sem=recv_sem,
            device_id=d,
            device_id_type=LOGICAL,
        ).start()

    pl.semaphore_wait(barrier, jnp.where(is_late, early, early - 1))
    each(0, lead, lambda d: pl.when(me != d)(lambda: start(d)))
    pl.when(is_late)(lambda: each(0, early, lambda d: signal(gate, d)))
    pack(lead, n - lead)
    each(lead, early, lambda d: pl.when(me != d)(lambda: start(d)))
    pl.semaphore_wait(gate, jnp.where(is_late, 1, late))
    each(early, n, lambda d: pl.when(me == d - late)(lambda: signal(gate, d)))
    each(early, n, lambda d: pl.when(me != d)(lambda: start(d)))
    recv[me] = send[me]
    sent = send.at[pl.ds(0, n - 1), pl.ds(0, sent_rows)]
    pltpu.make_async_copy(sent, sent, send_sem).wait()
    landed = recv.at[pl.ds(0, n - 1), pl.ds(0, sent_rows)]
    pltpu.make_async_copy(landed, landed, recv_sem).wait()

    data = recv[...].astype(jnp.float32)
    values = data[:, :stride].reshape(n * stride, width).astype(jnp.bfloat16)
    tags = data[:, stride:]
    per = goals // stride
    r_sub = lax.broadcasted_iota(jnp.int32, (BINS_DEV, goals), 0)
    r_lane = lax.broadcasted_iota(jnp.int32, (BINS_DEV, goals), 1)
    bin_of = r_sub.astype(jnp.float32)
    masses, chosen, totals = [], [], []
    for q in range(0, n, per):
        added = tree([tags[s] for s in range(q, min(q + per, n))])
        hit = bin_of == added[0:1]
        chosen.append(jnp.where(hit, 1.0, 0.0).astype(jnp.bfloat16))
        masses.append(jnp.where(hit, added[1:2] + added[2:3], 0.0))
        totals.append(added[3:4])
    choose = jnp.concatenate(chosen, axis=1)[:, : n * stride]
    sums = jnp.dot(choose, values, preferred_element_type=jnp.float32)
    mass_col = jnp.sum(tree(masses), axis=1, keepdims=True) + 1.0
    total = jnp.sum(tree(totals), axis=1, keepdims=True)
    mean_ref[...] = sums * (1.0 / mass_col)
    mass_row = jnp.sum(jnp.where(r_sub == r_lane, mass_col, 0.0), axis=0, keepdims=True)
    rarity_ref[...] = (jnp.log(total / (BINS_DEV * n)) - jnp.log(mass_row))[:, :BINS_DEV]


def put(mean, rarity, mean_hbm, rarity_hbm, sem):
    copies = [pltpu.make_async_copy(mean, mean_hbm, sem.at[0]), pltpu.make_async_copy(rarity, rarity_hbm, sem.at[1])]
    for c in copies:
        c.start()
    for c in copies:
        c.wait()


def shards(goal_embed, goal_bins, goal_weights):
    goals, width = goal_embed.shape
    across = lax.axis_size("gx")
    along = lax.axis_size("gy")
    n = across * along
    capacity = max(2, 2 * goals // n)
    stride = -(-capacity // 8) * 8
    mean, rarity = pl.pallas_call(
        functools.partial(kernel, across, along, stride),
        out_shape=(
            pltpu.VMEM((BINS_DEV, width), jnp.float32),
            pltpu.VMEM((1, BINS_DEV), jnp.float32),
        ),
        in_specs=[pl.BlockSpec(memory_space=pl.ANY)] * 3,
        out_specs=(pl.BlockSpec(memory_space=pltpu.VMEM),) * 2,
        scratch_shapes=[
            pltpu.VMEM((n, 2 * stride, width), jnp.bfloat16),
            pltpu.VMEM((n, 2 * stride, width), jnp.bfloat16),
            pltpu.SemaphoreType.DMA,
            pltpu.SemaphoreType.DMA,
            pltpu.SemaphoreType.REGULAR,
            pltpu.VMEM((goals, width), jnp.bfloat16),
            pltpu.VMEM((2, goals), jnp.float32),
            pltpu.SemaphoreType.DMA,
            pltpu.VMEM((1, goals), jnp.int32),
            pltpu.VMEM((1, goals), jnp.float32),
        ],
        compiler_params=pltpu.CompilerParams(collective_id=0, has_side_effects=True),
    )(goal_embed, goal_bins.reshape(1, goals), goal_weights.reshape(1, goals))
    mean, rarity = pl.pallas_call(
        put,
        out_shape=(
            jax.ShapeDtypeStruct((BINS_DEV, width), jnp.float32),
            jax.ShapeDtypeStruct((1, BINS_DEV), jnp.float32),
        ),
        in_specs=[pl.BlockSpec(memory_space=pltpu.VMEM)] * 2,
        out_specs=(pl.BlockSpec(memory_space=pl.ANY),) * 2,
        scratch_shapes=[pltpu.SemaphoreType.DMA((2,))],
    )(pltpu.with_memory_space_constraint(mean, pltpu.VMEM), pltpu.with_memory_space_constraint(rarity, pltpu.VMEM))
    return mean, rarity.reshape(BINS_DEV)


def solution(mesh):
    in_specs = (P(("gx", "gy"), None), P(("gx", "gy")), P(("gx", "gy")))
    out_specs = (P(("gx", "gy"), None), P(("gx", "gy")))
    return jax.shard_map(shards, mesh=mesh, in_specs=in_specs, out_specs=out_specs, check_vma=False)
```

```python
import functools

import jax
import jax.numpy as jnp
from jax import lax
from jax.experimental import pallas as pl
from jax.experimental.pallas import tpu as pltpu
from jax.sharding import PartitionSpec as P

BINS_DEV = 64
MARKS = 4
LATE = 6
LEAD = 8
LOGICAL = pl.DeviceIdType.LOGICAL


def each(first, last, body):
    if last - first <= 64:
        for k in range(first, last):
            body(k)
    else:
        lax.fori_loop(first, last, lambda k, c: (body(k), c)[1], 0)


def split2(x):
    hi = x.astype(jnp.bfloat16).astype(jnp.float32)
    return hi, x - hi


def split3(x):
    hi, rest = split2(x)
    mid, low = split2(rest)
    return hi, mid, low


def tree(parts):
    while len(parts) > 1:
        parts = [sum(parts[i : i + 2]) for i in range(0, len(parts), 2)]
    return parts[0]


def kernel(across, along, stride, embed_hbm, bins_hbm, weights_hbm, mean_ref, rarity_ref, send, recv, send_sem, recv_sem, gate, embed_ref, pair_ref, in_sem, bins_ref, weights_ref):
    n = across * along
    goals, width = embed_ref.shape
    embed_load = pltpu.make_async_copy(embed_hbm, embed_ref, send_sem)
    embed_load.start()
    pltpu.make_async_copy(bins_hbm, bins_ref, in_sem).start()
    pltpu.make_async_copy(weights_hbm, weights_ref, in_sem).start()
    sent_rows = stride + MARKS
    me = lax.axis_index("gx") * along + lax.axis_index("gy")
    late = min(LATE, n // 2)
    early = n - late
    is_late = me >= early

    def signal(sem, d):
        pl.semaphore_signal(sem, inc=1, device_id=d, device_id_type=LOGICAL)

    barrier = pltpu.get_barrier_semaphore()
    each(0, n, lambda d: pl.when((me != d) & (me < early))(lambda: signal(barrier, d)))

    shift = BINS_DEV.bit_length() - 1
    sub = lax.broadcasted_iota(jnp.int32, (goals, goals), 0)
    lane = lax.broadcasted_iota(jnp.int32, (goals, goals), 1)
    t_sub = lax.broadcasted_iota(jnp.int32, (stride, goals), 0)
    t_lane = lax.broadcasted_iota(jnp.int32, (stride, goals), 1)
    exact = jnp.bfloat16 if n <= 256 else jnp.float32
    before = (sub < lane).astype(exact)
    pltpu.make_async_copy(pair_ref, pair_ref, in_sem).wait()
    bins = bins_ref[...]
    weights = weights_ref[...]
    owners = lax.shift_right_logical(bins, shift)
    labels = (bins - owners * BINS_DEV).astype(jnp.float32)
    hi, lo = split2(weights)
    owners_row = jnp.broadcast_to(owners.astype(jnp.float32), (goals, goals)).astype(exact)
    same = jnp.where(owners_row.T == owners_row, before, exact(0))
    same = tree([same[i : i + 16] for i in range(0, goals, 16)])
    place = jnp.sum(same.astype(jnp.float32), axis=0, keepdims=True).astype(jnp.int32)
    weights_col = jnp.broadcast_to(weights, (goals, goals)).T
    embed_load.wait()
    base = lax.rem(me, goals // stride) * stride
    spot = (sub == place + base).astype(jnp.bfloat16)
    slot = owners * stride + place
    kind = lax.rem(t_sub, MARKS)
    kinds = jnp.where(kind == 0, labels, jnp.where(kind == 1, hi, jnp.where(kind == 2, lo, 0.0)))
    scaled = (weights_col[:, :width] * embed_ref[...].astype(jnp.float32)).astype(jnp.bfloat16)
    local = jnp.sum(weights, axis=1, keepdims=True)
    total = jnp.zeros((stride, goals), jnp.float32)
    for i, part in enumerate(split3(local)):
        total = jnp.where((t_sub == 3) & (t_lane == i), part, total)

    def pack(first, count):
        half = count // 2
        rows_iota = lax.broadcasted_iota(jnp.int32, (count * stride, goals), 0) + first * stride
        rows = jnp.dot((rows_iota == slot).astype(jnp.bfloat16), scaled, preferred_element_type=jnp.float32)
        owner_of = jnp.where(t_sub < MARKS, first, first + half)
        tagged = [jnp.where(owner_of + o == owners, kinds, 0.0) for o in range(half)]
        tagged = jnp.concatenate(tagged, axis=0).astype(jnp.bfloat16)
        marks = lax.dot_general(tagged, spot, (((1,), (1,)), ((), ())), preferred_element_type=jnp.float32)
        marks = marks.reshape(half, stride, goals)
        marks = jnp.concatenate([marks, jnp.roll(marks, -MARKS, axis=1)], axis=0) + total[None]
        both = jnp.concatenate([rows.reshape(count, stride, width), marks], axis=1)
        send[first : first + count] = both.astype(jnp.bfloat16)

    lead = min(LEAD, early)
    pack(0, lead)

    def start(d):
        pltpu.make_async_remote_copy(
            src_ref=send.at[d, pl.ds(0, sent_rows)],
            dst_ref=recv.at[me, pl.ds(0, sent_rows)],
            send_sem=send_sem,
            recv_sem=recv_sem,
            device_id=d,
            device_id_type=LOGICAL,
        ).start()

    pl.semaphore_wait(barrier, jnp.where(is_late, early, early - 1))
    each(0, lead, lambda d: pl.when(me != d)(lambda: start(d)))
    pl.when(is_late)(lambda: each(0, early, lambda d: signal(gate, d)))
    pack(lead, n - lead)
    each(lead, early, lambda d: pl.when(me != d)(lambda: start(d)))
    pl.semaphore_wait(gate, jnp.where(is_late, 1, late))
    each(early, n, lambda d: pl.when(me == d - late)(lambda: signal(gate, d)))
    each(early, n, lambda d: pl.when(me != d)(lambda: start(d)))
    recv[me] = send[me]
    landed = recv.at[pl.ds(0, n - 1), pl.ds(0, sent_rows)]
    pltpu.make_async_copy(landed, landed, recv_sem).wait()

    data = recv[...].astype(jnp.float32)
    values = data[:, :stride].reshape(n * stride, width).astype(jnp.bfloat16)
    tags = data[:, stride:]
    per = goals // stride
    r_sub = lax.broadcasted_iota(jnp.int32, (BINS_DEV, goals), 0)
    r_lane = lax.broadcasted_iota(jnp.int32, (BINS_DEV, goals), 1)
    bin_of = r_sub.astype(jnp.float32)
    masses, chosen, totals = [], [], []
    for q in range(0, n, per):
        added = tree([tags[s] for s in range(q, min(q + per, n))])
        hit = bin_of == added[0:1]
        chosen.append(jnp.where(hit, 1.0, 0.0).astype(jnp.bfloat16))
        masses.append(jnp.where(hit, added[1:2] + added[2:3], 0.0))
        totals.append(added[3:4])
    choose = jnp.concatenate(chosen, axis=1)[:, : n * stride]
    sums = jnp.dot(choose, values, preferred_element_type=jnp.float32)
    mass_col = jnp.sum(tree(masses), axis=1, keepdims=True) + 1.0
    total = jnp.sum(tree(totals), axis=1, keepdims=True)
    mean_ref[...] = sums * (1.0 / mass_col)
    mass_row = jnp.sum(jnp.where(r_sub == r_lane, mass_col, 0.0), axis=0, keepdims=True)
    rarity_ref[...] = (jnp.log(total / (BINS_DEV * n)) - jnp.log(mass_row))[:, :BINS_DEV]
    sent = send.at[pl.ds(0, n - 1), pl.ds(0, sent_rows)]
    pltpu.make_async_copy(sent, sent, send_sem).wait()


def put(mean, rarity, mean_hbm, rarity_hbm, sem):
    copies = [pltpu.make_async_copy(mean, mean_hbm, sem.at[0]), pltpu.make_async_copy(rarity, rarity_hbm, sem.at[1])]
    for c in copies:
        c.start()
    for c in copies:
        c.wait()


def shards(goal_embed, goal_bins, goal_weights):
    goals, width = goal_embed.shape
    across = lax.axis_size("gx")
    along = lax.axis_size("gy")
    n = across * along
    capacity = max(2, 2 * goals // n)
    stride = -(-capacity // 8) * 8
    mean, rarity = pl.pallas_call(
        functools.partial(kernel, across, along, stride),
        out_shape=(
            pltpu.VMEM((BINS_DEV, width), jnp.float32),
            pltpu.VMEM((1, BINS_DEV), jnp.float32),
        ),
        in_specs=[pl.BlockSpec(memory_space=pl.ANY)] * 3,
        out_specs=(pl.BlockSpec(memory_space=pltpu.VMEM),) * 2,
        scratch_shapes=[
            pltpu.VMEM((n, 2 * stride, width), jnp.bfloat16),
            pltpu.VMEM((n, 2 * stride, width), jnp.bfloat16),
            pltpu.SemaphoreType.DMA,
            pltpu.SemaphoreType.DMA,
            pltpu.SemaphoreType.REGULAR,
            pltpu.VMEM((goals, width), jnp.bfloat16),
            pltpu.VMEM((2, goals), jnp.float32),
            pltpu.SemaphoreType.DMA,
            pltpu.VMEM((1, goals), jnp.int32),
            pltpu.VMEM((1, goals), jnp.float32),
        ],
        compiler_params=pltpu.CompilerParams(collective_id=0, has_side_effects=True),
    )(goal_embed, goal_bins.reshape(1, goals), goal_weights.reshape(1, goals))
    mean, rarity = pl.pallas_call(
        put,
        out_shape=(
            jax.ShapeDtypeStruct((BINS_DEV, width), jnp.float32),
            jax.ShapeDtypeStruct((1, BINS_DEV), jnp.float32),
        ),
        in_specs=[pl.BlockSpec(memory_space=pltpu.VMEM)] * 2,
        out_specs=(pl.BlockSpec(memory_space=pl.ANY),) * 2,
        scratch_shapes=[pltpu.SemaphoreType.DMA((2,))],
    )(pltpu.with_memory_space_constraint(mean, pltpu.VMEM), pltpu.with_memory_space_constraint(rarity, pltpu.VMEM))
    return mean, rarity.reshape(BINS_DEV)


def solution(mesh):
    in_specs = (P(("gx", "gy"), None), P(("gx", "gy")), P(("gx", "gy")))
    out_specs = (P(("gx", "gy"), None), P(("gx", "gy")))
    return jax.shard_map(shards, mesh=mesh, in_specs=in_specs, out_specs=out_specs, check_vma=False)
```

```python
import functools

import jax
import jax.numpy as jnp
from jax import lax
from jax.experimental import pallas as pl
from jax.experimental.pallas import tpu as pltpu
from jax.sharding import PartitionSpec as P

BINS_DEV = 64
MARKS = 4
LATE = 6
LEAD = 8
LOGICAL = pl.DeviceIdType.LOGICAL


def each(first, last, body):
    if last - first <= 64:
        for k in range(first, last):
            body(k)
    else:
        lax.fori_loop(first, last, lambda k, c: (body(k), c)[1], 0)


def split2(x):
    hi = x.astype(jnp.bfloat16).astype(jnp.float32)
    return hi, x - hi


def split3(x):
    hi, rest = split2(x)
    mid, low = split2(rest)
    return hi, mid, low


def tree(parts):
    while len(parts) > 1:
        parts = [sum(parts[i : i + 2]) for i in range(0, len(parts), 2)]
    return parts[0]


def kernel(across, along, stride, embed_hbm, bins_hbm, weights_hbm, mean_ref, rarity_ref, send, recv, send_sem, recv_sem, gate, embed_ref, pair_ref, in_sem, bins_ref, weights_ref):
    n = across * along
    goals, width = embed_ref.shape
    for i in range(1):
        part = pl.ds(i * (goals // 1), goals // 1)
        pltpu.make_async_copy(embed_hbm.at[part], embed_ref.at[part], send_sem).start()
    pltpu.make_async_copy(bins_hbm, bins_ref, in_sem).start()
    pltpu.make_async_copy(weights_hbm, weights_ref, in_sem).start()
    embed_load = pltpu.make_async_copy(embed_hbm, embed_ref, send_sem)
    sent_rows = stride + MARKS
    me = lax.axis_index("gx") * along + lax.axis_index("gy")
    late = min(LATE, n // 2)
    early = n - late
    is_late = me >= early

    def signal(sem, d):
        pl.semaphore_signal(sem, inc=1, device_id=d, device_id_type=LOGICAL)

    barrier = pltpu.get_barrier_semaphore()
    each(0, n, lambda d: pl.when((me != d) & (me < early))(lambda: signal(barrier, d)))

    shift = BINS_DEV.bit_length() - 1
    sub = lax.broadcasted_iota(jnp.int32, (goals, goals), 0)
    lane = lax.broadcasted_iota(jnp.int32, (goals, goals), 1)
    t_sub = lax.broadcasted_iota(jnp.int32, (stride, goals), 0)
    t_lane = lax.broadcasted_iota(jnp.int32, (stride, goals), 1)
    exact = jnp.bfloat16 if n <= 256 else jnp.float32
    before = (sub < lane).astype(exact)
    pltpu.make_async_copy(pair_ref, pair_ref, in_sem).wait()
    bins = bins_ref[...]
    weights = weights_ref[...]
    owners = lax.shift_right_logical(bins, shift)
    labels = (bins - owners * BINS_DEV).astype(jnp.float32)
    hi, lo = split2(weights)
    owners_row = jnp.broadcast_to(owners.astype(jnp.float32), (goals, goals)).astype(exact)
    same = jnp.where(owners_row.T == owners_row, before, exact(0))
    same = tree([same[i : i + 16] for i in range(0, goals, 16)])
    place = jnp.sum(same.astype(jnp.float32), axis=0, keepdims=True).astype(jnp.int32)
    weights_col = jnp.broadcast_to(weights, (goals, goals)).T
    embed_load.wait()
    base = lax.rem(me, goals // stride) * stride
    spot = (sub == place + base).astype(jnp.bfloat16)
    slot = owners * stride + place
    kind = lax.rem(t_sub, MARKS)
    kinds = jnp.where(kind == 0, labels, jnp.where(kind == 1, hi, jnp.where(kind == 2, lo, 0.0)))
    scaled = (weights_col[:, :width] * embed_ref[...].astype(jnp.float32)).astype(jnp.bfloat16)
    local = jnp.sum(weights, axis=1, keepdims=True)
    total = jnp.zeros((stride, goals), jnp.float32)
    for i, part in enumerate(split3(local)):
        total = jnp.where((t_sub == 3) & (t_lane == i), part, total)

    def pack(first, count):
        half = count // 2
        rows_iota = lax.broadcasted_iota(jnp.int32, (count * stride, goals), 0) + first * stride
        rows = jnp.dot((rows_iota == slot).astype(jnp.bfloat16), scaled, preferred_element_type=jnp.float32)
        owner_of = jnp.where(t_sub < MARKS, first, first + half)
        tagged = [jnp.where(owner_of + o == owners, kinds, 0.0) for o in range(half)]
        tagged = jnp.concatenate(tagged, axis=0).astype(jnp.bfloat16)
        marks = lax.dot_general(tagged, spot, (((1,), (1,)), ((), ())), preferred_element_type=jnp.float32)
        marks = marks.reshape(half, stride, goals)
        marks = jnp.concatenate([marks, jnp.roll(marks, -MARKS, axis=1)], axis=0) + total[None]
        both = jnp.concatenate([rows.reshape(count, stride, width), marks], axis=1)
        send[first : first + count] = both.astype(jnp.bfloat16)

    lead = min(LEAD, early)
    pack(0, lead)

    def start(d):
        pltpu.make_async_remote_copy(
            src_ref=send.at[d, pl.ds(0, sent_rows)],
            dst_ref=recv.at[me, pl.ds(0, sent_rows)],
            send_sem=send_sem,
            recv_sem=recv_sem,
            device_id=d,
            device_id_type=LOGICAL,
        ).start()

    pl.semaphore_wait(barrier, jnp.where(is_late, early, early - 1))
    pl.when(is_late)(lambda: each(0, early, lambda d: signal(gate, d)))
    each(0, lead, lambda d: pl.when(me != d)(lambda: start(d)))
    pack(lead, n - lead)
    each(lead, early, lambda d: pl.when(me != d)(lambda: start(d)))
    pl.semaphore_wait(gate, jnp.where(is_late, 1, late))
    each(early, n, lambda d: pl.when(me == d - late)(lambda: signal(gate, d)))
    each(early, n, lambda d: pl.when(me != d)(lambda: start(d)))
    recv[me] = send[me]
    sent = send.at[pl.ds(0, n - 1), pl.ds(0, sent_rows)]
    pltpu.make_async_copy(sent, sent, send_sem).wait()
    landed = recv.at[pl.ds(0, n - 1), pl.ds(0, sent_rows)]
    pltpu.make_async_copy(landed, landed, recv_sem).wait()

    data = recv[...].astype(jnp.float32)
    values = data[:, :stride].reshape(n * stride, width).astype(jnp.bfloat16)
    tags = data[:, stride:]
    per = goals // stride
    r_sub = lax.broadcasted_iota(jnp.int32, (BINS_DEV, goals), 0)
    r_lane = lax.broadcasted_iota(jnp.int32, (BINS_DEV, goals), 1)
    bin_of = r_sub.astype(jnp.float32)
    masses, chosen, totals = [], [], []
    for q in range(0, n, per):
        added = tree([tags[s] for s in range(q, min(q + per, n))])
        hit = bin_of == added[0:1]
        chosen.append(jnp.where(hit, 1.0, 0.0).astype(jnp.bfloat16))
        masses.append(jnp.where(hit, added[1:2] + added[2:3], 0.0))
        totals.append(added[3:4])
    choose = jnp.concatenate(chosen, axis=1)[:, : n * stride]
    sums = jnp.dot(choose, values, preferred_element_type=jnp.float32)
    mass_col = jnp.sum(tree(masses), axis=1, keepdims=True) + 1.0
    total = jnp.sum(tree(totals), axis=1, keepdims=True)
    mean_ref[...] = sums * (1.0 / mass_col)
    mass_row = jnp.sum(jnp.where(r_sub == r_lane, mass_col, 0.0), axis=0, keepdims=True)
    rarity_ref[...] = (jnp.log(total / (BINS_DEV * n)) - jnp.log(mass_row))[:, :BINS_DEV]


def put(mean, rarity, mean_hbm, rarity_hbm, sem):
    copies = [pltpu.make_async_copy(mean, mean_hbm, sem.at[0]), pltpu.make_async_copy(rarity, rarity_hbm, sem.at[1])]
    for c in copies:
        c.start()
    for c in copies:
        c.wait()


def shards(goal_embed, goal_bins, goal_weights):
    goals, width = goal_embed.shape
    across = lax.axis_size("gx")
    along = lax.axis_size("gy")
    n = across * along
    capacity = max(2, 2 * goals // n)
    stride = -(-capacity // 8) * 8
    mean, rarity = pl.pallas_call(
        functools.partial(kernel, across, along, stride),
        out_shape=(
            pltpu.VMEM((BINS_DEV, width), jnp.float32),
            pltpu.VMEM((1, BINS_DEV), jnp.float32),
        ),
        in_specs=[pl.BlockSpec(memory_space=pl.ANY)] * 3,
        out_specs=(pl.BlockSpec(memory_space=pltpu.VMEM),) * 2,
        scratch_shapes=[
            pltpu.VMEM((n, 2 * stride, width), jnp.bfloat16),
            pltpu.VMEM((n, 2 * stride, width), jnp.bfloat16),
            pltpu.SemaphoreType.DMA,
            pltpu.SemaphoreType.DMA,
            pltpu.SemaphoreType.REGULAR,
            pltpu.VMEM((goals, width), jnp.bfloat16),
            pltpu.VMEM((2, goals), jnp.float32),
            pltpu.SemaphoreType.DMA,
            pltpu.VMEM((1, goals), jnp.int32),
            pltpu.VMEM((1, goals), jnp.float32),
        ],
        compiler_params=pltpu.CompilerParams(collective_id=0, has_side_effects=True),
    )(goal_embed, goal_bins.reshape(1, goals), goal_weights.reshape(1, goals))
    mean, rarity = pl.pallas_call(
        put,
        out_shape=(
            jax.ShapeDtypeStruct((BINS_DEV, width), jnp.float32),
            jax.ShapeDtypeStruct((1, BINS_DEV), jnp.float32),
        ),
        in_specs=[pl.BlockSpec(memory_space=pltpu.VMEM)] * 2,
        out_specs=(pl.BlockSpec(memory_space=pl.ANY),) * 2,
        scratch_shapes=[pltpu.SemaphoreType.DMA((2,))],
    )(pltpu.with_memory_space_constraint(mean, pltpu.VMEM), pltpu.with_memory_space_constraint(rarity, pltpu.VMEM))
    return mean, rarity.reshape(BINS_DEV)


def solution(mesh):
    in_specs = (P(("gx", "gy"), None), P(("gx", "gy")), P(("gx", "gy")))
    out_specs = (P(("gx", "gy"), None), P(("gx", "gy")))
    return jax.shard_map(shards, mesh=mesh, in_specs=in_specs, out_specs=out_specs, check_vma=False)
```

```python
import functools

import jax
import jax.numpy as jnp
from jax import lax
from jax.experimental import pallas as pl
from jax.experimental.pallas import tpu as pltpu
from jax.sharding import PartitionSpec as P

BINS_DEV = 64
MARKS = 4
LATE = 6
LEAD = 16
LOGICAL = pl.DeviceIdType.LOGICAL


def each(first, last, body):
    if last - first <= 64:
        for k in range(first, last):
            body(k)
    else:
        lax.fori_loop(first, last, lambda k, c: (body(k), c)[1], 0)


def split2(x):
    hi = x.astype(jnp.bfloat16).astype(jnp.float32)
    return hi, x - hi


def split3(x):
    hi, rest = split2(x)
    mid, low = split2(rest)
    return hi, mid, low


def tree(parts):
    while len(parts) > 1:
        parts = [sum(parts[i : i + 2]) for i in range(0, len(parts), 2)]
    return parts[0]


def kernel(across, along, stride, embed_hbm, bins_hbm, weights_hbm, mean_ref, rarity_ref, send, recv, send_sem, recv_sem, gate, embed_ref, pair_ref, in_sem, bins_ref, weights_ref):
    n = across * along
    goals, width = embed_ref.shape
    for i in range(1):
        part = pl.ds(i * (goals // 1), goals // 1)
        pltpu.make_async_copy(embed_hbm.at[part], embed_ref.at[part], send_sem).start()
    pltpu.make_async_copy(bins_hbm, bins_ref, in_sem).start()
    pltpu.make_async_copy(weights_hbm, weights_ref, in_sem).start()
    embed_load = pltpu.make_async_copy(embed_hbm, embed_ref, send_sem)
    sent_rows = stride + MARKS
    me = lax.axis_index("gx") * along + lax.axis_index("gy")
    late = min(LATE, n // 2)
    early = n - late
    is_late = me >= early

    def signal(sem, d):
        pl.semaphore_signal(sem, inc=1, device_id=d, device_id_type=LOGICAL)

    barrier = pltpu.get_barrier_semaphore()
    each(0, n, lambda d: pl.when((me != d) & (me < early))(lambda: signal(barrier, d)))

    shift = BINS_DEV.bit_length() - 1
    sub = lax.broadcasted_iota(jnp.int32, (goals, goals), 0)
    lane = lax.broadcasted_iota(jnp.int32, (goals, goals), 1)
    t_sub = lax.broadcasted_iota(jnp.int32, (stride, goals), 0)
    t_lane = lax.broadcasted_iota(jnp.int32, (stride, goals), 1)
    exact = jnp.bfloat16 if n <= 256 else jnp.float32
    before = (sub < lane).astype(exact)
    pltpu.make_async_copy(pair_ref, pair_ref, in_sem).wait()
    bins = bins_ref[...]
    weights = weights_ref[...]
    owners = lax.shift_right_logical(bins, shift)
    labels = (bins - owners * BINS_DEV).astype(jnp.float32)
    hi, lo = split2(weights)
    owners_row = jnp.broadcast_to(owners.astype(jnp.float32), (goals, goals)).astype(exact)
    same = jnp.where(owners_row.T == owners_row, before, exact(0))
    same = tree([same[i : i + 16] for i in range(0, goals, 16)])
    place = jnp.sum(same.astype(jnp.float32), axis=0, keepdims=True).astype(jnp.int32)
    weights_col = jnp.broadcast_to(weights, (goals, goals)).T
    embed_load.wait()
    base = lax.rem(me, goals // stride) * stride
    spot = (sub == place + base).astype(jnp.bfloat16)
    slot = owners * stride + place
    kind = lax.rem(t_sub, MARKS)
    kinds = jnp.where(kind == 0, labels, jnp.where(kind == 1, hi, jnp.where(kind == 2, lo, 0.0)))
    scaled = (weights_col[:, :width] * embed_ref[...].astype(jnp.float32)).astype(jnp.bfloat16)
    local = jnp.sum(weights, axis=1, keepdims=True)
    total = jnp.zeros((stride, goals), jnp.float32)
    for i, part in enumerate(split3(local)):
        total = jnp.where((t_sub == 3) & (t_lane == i), part, total)

    def pack(first, count):
        half = count // 2
        rows_iota = lax.broadcasted_iota(jnp.int32, (count * stride, goals), 0) + first * stride
        rows = jnp.dot((rows_iota == slot).astype(jnp.bfloat16), scaled, preferred_element_type=jnp.float32)
        owner_of = jnp.where(t_sub < MARKS, first, first + half)
        tagged = [jnp.where(owner_of + o == owners, kinds, 0.0) for o in range(half)]
        tagged = jnp.concatenate(tagged, axis=0).astype(jnp.bfloat16)
        marks = lax.dot_general(tagged, spot, (((1,), (1,)), ((), ())), preferred_element_type=jnp.float32)
        marks = marks.reshape(half, stride, goals)
        marks = jnp.concatenate([marks, jnp.roll(marks, -MARKS, axis=1)], axis=0) + total[None]
        both = jnp.concatenate([rows.reshape(count, stride, width), marks], axis=1)
        send[first : first + count] = both.astype(jnp.bfloat16)

    lead = min(LEAD, early)
    pack(0, lead)

    def start(d):
        pltpu.make_async_remote_copy(
            src_ref=send.at[d, pl.ds(0, sent_rows)],
            dst_ref=recv.at[me, pl.ds(0, sent_rows)],
            send_sem=send_sem,
            recv_sem=recv_sem,
            device_id=d,
            device_id_type=LOGICAL,
        ).start()

    pl.semaphore_wait(barrier, jnp.where(is_late, early, early - 1))
    each(0, lead, lambda d: pl.when(me != d)(lambda: start(d)))
    pl.when(is_late)(lambda: each(0, early, lambda d: signal(gate, d)))
    pack(lead, n - lead)
    each(lead, early, lambda d: pl.when(me != d)(lambda: start(d)))
    pl.semaphore_wait(gate, jnp.where(is_late, 1, late))
    each(early, n, lambda d: pl.when(me == d - late)(lambda: signal(gate, d)))
    each(early, n, lambda d: pl.when(me != d)(lambda: start(d)))
    recv[me] = send[me]
    sent = send.at[pl.ds(0, n - 1), pl.ds(0, sent_rows)]
    pltpu.make_async_copy(sent, sent, send_sem).wait()
    landed = recv.at[pl.ds(0, n - 1), pl.ds(0, sent_rows)]
    pltpu.make_async_copy(landed, landed, recv_sem).wait()

    data = recv[...].astype(jnp.float32)
    values = data[:, :stride].reshape(n * stride, width).astype(jnp.bfloat16)
    tags = data[:, stride:]
    per = goals // stride
    r_sub = lax.broadcasted_iota(jnp.int32, (BINS_DEV, goals), 0)
    r_lane = lax.broadcasted_iota(jnp.int32, (BINS_DEV, goals), 1)
    bin_of = r_sub.astype(jnp.float32)
    masses, chosen, totals = [], [], []
    for q in range(0, n, per):
        added = tree([tags[s] for s in range(q, min(q + per, n))])
        hit = bin_of == added[0:1]
        chosen.append(jnp.where(hit, 1.0, 0.0).astype(jnp.bfloat16))
        masses.append(jnp.where(hit, added[1:2] + added[2:3], 0.0))
        totals.append(added[3:4])
    choose = jnp.concatenate(chosen, axis=1)[:, : n * stride]
    sums = jnp.dot(choose, values, preferred_element_type=jnp.float32)
    mass_col = jnp.sum(tree(masses), axis=1, keepdims=True) + 1.0
    total = jnp.sum(tree(totals), axis=1, keepdims=True)
    mean_ref[...] = sums * (1.0 / mass_col)
    mass_row = jnp.sum(jnp.where(r_sub == r_lane, mass_col, 0.0), axis=0, keepdims=True)
    rarity_ref[...] = (jnp.log(total / (BINS_DEV * n)) - jnp.log(mass_row))[:, :BINS_DEV]


def put(mean, rarity, mean_hbm, rarity_hbm, sem):
    copies = [pltpu.make_async_copy(mean, mean_hbm, sem.at[0]), pltpu.make_async_copy(rarity, rarity_hbm, sem.at[1])]
    for c in copies:
        c.start()
    for c in copies:
        c.wait()


def shards(goal_embed, goal_bins, goal_weights):
    goals, width = goal_embed.shape
    across = lax.axis_size("gx")
    along = lax.axis_size("gy")
    n = across * along
    capacity = max(2, 2 * goals // n)
    stride = -(-capacity // 8) * 8
    mean, rarity = pl.pallas_call(
        functools.partial(kernel, across, along, stride),
        out_shape=(
            pltpu.VMEM((BINS_DEV, width), jnp.float32),
            pltpu.VMEM((1, BINS_DEV), jnp.float32),
        ),
        in_specs=[pl.BlockSpec(memory_space=pl.ANY)] * 3,
        out_specs=(pl.BlockSpec(memory_space=pltpu.VMEM),) * 2,
        scratch_shapes=[
            pltpu.VMEM((n, 2 * stride, width), jnp.bfloat16),
            pltpu.VMEM((n, 2 * stride, width), jnp.bfloat16),
            pltpu.SemaphoreType.DMA,
            pltpu.SemaphoreType.DMA,
            pltpu.SemaphoreType.REGULAR,
            pltpu.VMEM((goals, width), jnp.bfloat16),
            pltpu.VMEM((2, goals), jnp.float32),
            pltpu.SemaphoreType.DMA,
            pltpu.VMEM((1, goals), jnp.int32),
            pltpu.VMEM((1, goals), jnp.float32),
        ],
        compiler_params=pltpu.CompilerParams(collective_id=0, has_side_effects=True),
    )(goal_embed, goal_bins.reshape(1, goals), goal_weights.reshape(1, goals))
    mean, rarity = pl.pallas_call(
        put,
        out_shape=(
            jax.ShapeDtypeStruct((BINS_DEV, width), jnp.float32),
            jax.ShapeDtypeStruct((1, BINS_DEV), jnp.float32),
        ),
        in_specs=[pl.BlockSpec(memory_space=pltpu.VMEM)] * 2,
        out_specs=(pl.BlockSpec(memory_space=pl.ANY),) * 2,
        scratch_shapes=[pltpu.SemaphoreType.DMA((2,))],
    )(pltpu.with_memory_space_constraint(mean, pltpu.VMEM), pltpu.with_memory_space_constraint(rarity, pltpu.VMEM))
    return mean, rarity.reshape(BINS_DEV)


def solution(mesh):
    in_specs = (P(("gx", "gy"), None), P(("gx", "gy")), P(("gx", "gy")))
    out_specs = (P(("gx", "gy"), None), P(("gx", "gy")))
    return jax.shard_map(shards, mesh=mesh, in_specs=in_specs, out_specs=out_specs, check_vma=False)
```
